16 devices in a mesh: rep: 1, dp: 16 (over x, y, z, core).
Axes of the slice: x: 2, y: 2, z: 2, core: 2. Of those that a mesh axis runs over, the one named last changes fastest.
Arguments:
- x: bfloat16 [16, 2048, 896], P(('rep', 'dp'))
- dy: bfloat16 [16, 2048, 896], P(('rep', 'dp'))
- wq: bfloat16 [2, 896, 896], replicated
- wk: bfloat16 [2, 896, 128], replicated
- wv: bfloat16 [2, 896, 128], replicated
- wo: bfloat16 [2, 896, 896], replicated
- w_gate: bfloat16 [2, 896, 2560], replicated
- w_up: bfloat16 [2, 896, 2560], replicated
- w_down: bfloat16 [2, 2560, 896], replicated
- m_wq: float32 [2, 896, 896], P(None, 'dp')
- m_wk: float32 [2, 896, 128], P(None, 'dp')
- m_wv: float32 [2, 896, 128], P(None, 'dp')
- m_wo: float32 [2, 896, 896], P(None, 'dp')
- m_w_gate: float32 [2, 896, 2560], P(None, 'dp')
- m_w_up: float32 [2, 896, 2560], P(None, 'dp')
- m_w_down: float32 [2, 2560, 896], P(None, 'dp')
- v_wq: float32 [2, 896, 896], P(None, 'dp')
- v_wk: float32 [2, 896, 128], P(None, 'dp')
- v_wv: float32 [2, 896, 128], P(None, 'dp')
- v_wo: float32 [2, 896, 896], P(None, 'dp')
- v_w_gate: float32 [2, 896, 2560], P(None, 'dp')
- v_w_up: float32 [2, 896, 2560], P(None, 'dp')
- v_w_down: float32 [2, 2560, 896], P(None, 'dp')
Outputs:
- output 1: bfloat16 [2, 896, 896], P('rep')
- output 2: bfloat16 [2, 896, 128], P('rep')
- output 3: bfloat16 [2, 896, 128], P('rep')
- output 4: bfloat16 [2, 896, 896], P('rep')
- output 5: bfloat16 [2, 896, 2560], P('rep')
- output 6: bfloat16 [2, 896, 2560], P('rep')
- output 7: bfloat16 [2, 2560, 896], P('rep')
- output 8: float32 [2, 896, 896], P('rep', 'dp')
- output 9: float32 [2, 896, 128], P('rep', 'dp')
- output 10: float32 [2, 896, 128], P('rep', 'dp')
- output 11: float32 [2, 896, 896], P('rep', 'dp')
- output 12: float32 [2, 896, 2560], P('rep', 'dp')
- output 13: float32 [2, 896, 2560], P('rep', 'dp')
- output 14: float32 [2, 2560, 896], P('rep', 'dp')
- output 15: float32 [2, 896, 896], P('rep', 'dp')
- output 16: float32 [2, 896, 128], P('rep', 'dp')
- output 17: float32 [2, 896, 128], P('rep', 'dp')
- output 18: float32 [2, 896, 896], P('rep', 'dp')
- output 19: float32 [2, 896, 2560], P('rep', 'dp')
- output 20: float32 [2, 896, 2560], P('rep', 'dp')
- output 21: float32 [2, 2560, 896], P('rep', 'dp')
All inputs are finite; a program needn't handle non-finite values.
Results may differ from the reference program's by a relative error of at most 0.0291.
Values are sent between devices in bfloat16 or wider.
A program may use at most 2 GiB of HBM per device.

```python
import jax
import jax.numpy as jnp
from jax import lax

SEQUENCES = 16
TOKENS = 2048
D = 896
HEADS = 7
KV_HEADS = 1
HEAD = 128
FF = 2560
LAYERS = 2
THETA = 10000
NAMES = ("wq", "wk", "wv", "wo", "w_gate", "w_up", "w_down")
SHAPES = {
    "wq": (LAYERS, D, HEADS * HEAD),
    "wk": (LAYERS, D, KV_HEADS * HEAD),
    "wv": (LAYERS, D, KV_HEADS * HEAD),
    "wo": (LAYERS, HEADS * HEAD, D),
    "w_gate": (LAYERS, D, FF),
    "w_up": (LAYERS, D, FF),
    "w_down": (LAYERS, FF, D),
}


def bump(key, n, height):
    away = (jnp.arange(n, dtype=jnp.int32) - jax.random.randint(key, (), 0, n, jnp.int32)) % n
    return jnp.where(away < n // 8, height, 1.0)


def together(key, own, strength):
    shared = jax.random.normal(key, own.shape[1:], jnp.float32)
    return (own + strength * shared) * lax.rsqrt(1 + strength * strength)


def setup_inputs(seed: int = 0, part: int = 0) -> dict:
    kx, kdy, ka, kb, kz, kf, kh, kl, *keys = jax.random.split(jax.random.key(seed), 8 + 3 * len(NAMES))
    kx, kdy, ka, kb = (jax.random.fold_in(k, part) for k in (kx, kdy, ka, kb))
    kw, km, kv = (keys[i::3] for i in range(3))
    shape = (SEQUENCES, TOKENS, D)
    much_x, much_dy = jax.random.uniform(kz, (2,), jnp.float32, 0.0, 1.0)
    loud = 2.0 ** jax.random.uniform(jax.random.fold_in(kz, 1), (), jnp.float32, -1.0, 2.0)
    layers = 2.0 ** jax.random.uniform(kl, (LAYERS, 1, 1), jnp.float32, -1.0, 1.0)
    times = {"wq": 1.0, "wk": 1.0, "wv": 2.0, "wo": layers, "w_gate": 1.0, "w_up": bump(kh, FF, 4.0), "w_down": layers}
    x = together(ka, jax.random.normal(kx, shape, jnp.float32), much_x) * bump(kf, D, 4.0)
    dy = together(kb, jax.random.normal(kdy, shape, jnp.float32), much_dy)
    drawn = {"x": x.astype(jnp.bfloat16), "dy": (loud * dy * (SEQUENCES * TOKENS) ** -0.5).astype(jnp.bfloat16)}
    for key, name in zip(kw, NAMES, strict=True):
        drawn[name] = (jax.random.normal(key, SHAPES[name], jnp.float32) * SHAPES[name][1] ** -0.5 * times[name]).astype(jnp.bfloat16)
    for key, name in zip(km, NAMES, strict=True):
        drawn[f"m_{name}"] = 0.1 * jax.random.normal(key, SHAPES[name], jnp.float32)
    for key, name in zip(kv, NAMES, strict=True):
        drawn[f"v_{name}"] = jax.random.uniform(key, SHAPES[name], jnp.float32, 0.02, 0.06)
    return drawn


def matmul(a, w):
    return jnp.dot(a, w, preferred_element_type=jnp.float32).astype(jnp.bfloat16)


def normed(h):
    wide = h.astype(jnp.float32)
    scale = lax.rsqrt(jnp.mean(wide**2, -1, keepdims=True) + 1e-6)
    return (wide * scale).astype(jnp.bfloat16)


def turned(t, theta):
    half = t.shape[-1] // 2
    angle = jnp.arange(t.shape[0], dtype=jnp.float32)[:, None] * theta ** (-jnp.arange(half, dtype=jnp.float32) / half)
    cos, sin = jnp.cos(angle)[:, None], jnp.sin(angle)[:, None]
    a, b = t[..., :half].astype(jnp.float32), t[..., half:].astype(jnp.float32)
    return jnp.concatenate([a * cos - b * sin, b * cos + a * sin], -1).astype(jnp.bfloat16)


def seen_by(q, k, v):
    tokens, kv = q.shape[0], k.shape[1]
    q = q.reshape(tokens, kv, -1, q.shape[-1])
    scores = jnp.einsum("tgsd,ugd->gstu", q.astype(jnp.float32), k.astype(jnp.float32)) * q.shape[-1] ** -0.5
    place = jnp.arange(tokens)
    weights = jax.nn.softmax(jnp.where(place[:, None] >= place, scores, -jnp.inf), -1).astype(jnp.bfloat16)
    return jnp.einsum("gstu,ugd->tgsd", weights.astype(jnp.float32), v.astype(jnp.float32)).astype(jnp.bfloat16).reshape(tokens, -1)


def layer(h, w):
    a = normed(h)
    q, k = (turned(matmul(a, w[name]).reshape(h.shape[0], -1, HEAD), THETA) for name in ("wq", "wk"))
    h = h + matmul(seen_by(q, k, matmul(a, w["wv"]).reshape(h.shape[0], -1, HEAD)), w["wo"])
    b = normed(h)
    gate = jnp.dot(b, w["w_gate"], preferred_element_type=jnp.float32)
    up = jnp.dot(b, w["w_up"], preferred_element_type=jnp.float32)
    return h + matmul((jax.nn.silu(gate) * up).astype(jnp.bfloat16), w["w_down"])


def adamw(w, m, v, g):
    m = 0.9 * m + 0.1 * g
    v = 0.95 * v + 0.05 * g * g
    step = m * lax.rsqrt(v + 1e-8) + 0.1 * w
    return (w - 0.02 * step).astype(jnp.bfloat16), m, v


def clipped(gradients, sum_of_squares, count):
    factor = jnp.minimum(1.0, 0.5 * lax.rsqrt(sum_of_squares / count + 1e-30))
    return [g * factor for g in gradients]


def stack(weights, h):
    return lax.scan(lambda h, w: (layer(h, w), None), h, weights)[0]


def reference(x, dy, wq, wk, wv, wo, w_gate, w_up, w_down, m_wq, m_wk, m_wv, m_wo, m_w_gate, m_w_up, m_w_down, v_wq, v_wk, v_wv, v_wo, v_w_gate, v_w_up, v_w_down):
    weights = dict(zip(NAMES, (wq, wk, wv, wo, w_gate, w_up, w_down), strict=True))

    def take(so_far, sequence):
        h, by_y = sequence
        _, back = jax.vjp(stack, weights, h)
        by_weights, by_h = back(by_y)
        return jax.tree.map(lambda total, term: total + term.astype(jnp.float32), so_far, by_weights), by_h

    none_yet = {name: jnp.zeros(w.shape, jnp.float32) for name, w in weights.items()}
    by_weights, by_x = lax.scan(take, none_yet, (x, dy))
    gradients = [by_weights[name].astype(jnp.bfloat16).astype(jnp.float32) for name in NAMES]
    gradients = clipped(gradients, sum(jnp.sum(g * g) for g in gradients), sum(g.size for g in gradients))
    first = (m_wq, m_wk, m_wv, m_wo, m_w_gate, m_w_up, m_w_down)
    second = (v_wq, v_wk, v_wv, v_wo, v_w_gate, v_w_up, v_w_down)
    new = [adamw(weights[name].astype(jnp.float32), m, v, g) for name, m, v, g in zip(NAMES, first, second, gradients, strict=True)]
    return tuple(one[which] for which in range(3) for one in new)
```

```python
import functools

import jax
import jax.numpy as jnp
import numpy as np
from jax import lax
from jax.experimental import pallas as pl
from jax.experimental.pallas import tpu as pltpu
from jax.sharding import PartitionSpec as P

NEG = -1e30
LOG2E = 1.4426950408889634
VMEM = 56 * 2**20
HEAD = 128
THETA = 10000
NAMES = ("wq", "wk", "wv", "wo", "w_gate", "w_up", "w_down")
FWD_BLOCK, BWD_BLOCK = (512, 512), (512, 512)


def _fit(size, want, unit=128):
    return max(n for n in range(unit, max(min(want, size), unit) + 1, unit) if size % n == 0)


def _dot(a, b, ca, cb):
    return lax.dot_general(a, b, (((ca,), (cb,)), ((), ())), preferred_element_type=jnp.float32)


def tables(tokens):
    half = HEAD // 2
    angle = np.arange(tokens)[:, None] * float(THETA) ** (-np.arange(half) / half)
    cos, sin = np.cos(angle), np.sin(angle)
    return jnp.asarray(np.concatenate([cos, cos], 1), jnp.float32), jnp.asarray(np.concatenate([-sin, sin], 1), jnp.float32)


def _turned(t, cos, sin):
    wide = t.astype(jnp.float32)
    return (wide * cos + pltpu.roll(wide, HEAD // 2, 1) * sin).astype(jnp.bfloat16)


def _blocks(i, bq, bk):
    return lax.div(i * bq, bk), lax.div(i * bq + bq + bk - 1, bk)


def _lag(bk, bq):
    return lax.broadcasted_iota(jnp.int32, (bk, bq), 1) - lax.broadcasted_iota(jnp.int32, (bk, bq), 0)


def _attend(q_ref, k_ref, v_ref, cos_ref, sin_ref, o_ref, lse_ref, turned_ref, key_ref, values_s, top_s, mix_s, lag_s, *, bk):
    bq, heads = q_ref.shape[0], q_ref.shape[1] // HEAD
    i = pl.program_id(0)
    scale = HEAD**-0.5
    e = scale * LOG2E
    here = pl.ds(pl.multiple_of(i * bq, bq), bq)

    @pl.when(i == 0)
    def _():
        key_ref[...] = _turned(k_ref[...], cos_ref[...], sin_ref[...])
        values_s[:HEAD, :] = v_ref[...].T
        values_s[HEAD:, :] = jnp.ones((16, v_ref.shape[0]), jnp.bfloat16)
        lag_s[...] = _lag(bk, bq)

    cos, sin = cos_ref[here, :], sin_ref[here, :]
    for n in range(heads):
        turned_ref[n] = _turned(q_ref[:, n * HEAD : (n + 1) * HEAD], cos, sin)
    top_s[...] = jnp.full(top_s.shape, NEG, jnp.float32)
    mix_s[...] = jnp.zeros(mix_s.shape, jnp.float32)

    def block(j, masked):
        keys = pl.ds(pl.multiple_of(j * bk, bk), bk)
        scores = [_dot(key_ref[keys, :], turned_ref[n], 1, 1) for n in range(heads)]
        weights, keeps = [], []
        for n, s in enumerate(scores):
            if masked:
                s = jnp.where(lag_s[...] >= j * bk - i * bq, s, 2 * NEG)
            old = top_s[n : n + 1, :]
            top = jnp.maximum(old, s.max(axis=0, keepdims=True))
            top_s[n : n + 1, :] = top
            weights.append(jnp.exp2((s - top) * e).astype(jnp.bfloat16))
            keeps.append(jnp.exp2((old - top) * e))
        for n, (p, keep) in enumerate(zip(weights, keeps)):
            mix_s[n] = mix_s[n] * keep + _dot(values_s[:, keys], p, 1, 0)

    whole, last = _blocks(i, bq, bk)
    lax.fori_loop(0, whole, lambda j, _: block(j, False), None)
    lax.fori_loop(whole, last, lambda j, _: block(j, True), None)
    for n in range(heads):
        total = mix_s[n, HEAD : HEAD + 1, :]
        o_ref[:, n * HEAD : (n + 1) * HEAD] = (mix_s[n, :HEAD, :] * (1 / total)).T.astype(o_ref.dtype)
        lse_ref[n : n + 1, :] = top_s[n : n + 1, :] * e + jnp.log2(total)


def attend(qkv, turn):
    tokens, heads = qkv.shape[0], qkv.shape[1] // HEAD - 2
    bq, bk = FWD_BLOCK
    column = lambda n: pl.BlockSpec((tokens, HEAD), lambda i: (0, n))
    rows = pl.BlockSpec((bq, heads * HEAD), lambda i: (i, 0))
    return pl.pallas_call(
        functools.partial(_attend, bk=bk),
        grid=(tokens // bq,),
        in_specs=[rows, column(heads), column(heads + 1), column(0), column(0)],
        out_specs=[rows, pl.BlockSpec((heads, bq), lambda i: (0, i)), pl.BlockSpec((heads, bq, HEAD), lambda i: (0, i, 0)), column(0)],
        out_shape=[jax.ShapeDtypeStruct((tokens, heads * HEAD), jnp.bfloat16), jax.ShapeDtypeStruct((heads, tokens), jnp.float32),
                   jax.ShapeDtypeStruct((heads, tokens, HEAD), jnp.bfloat16), jax.ShapeDtypeStruct((tokens, HEAD), jnp.bfloat16)],
        scratch_shapes=[pltpu.VMEM((HEAD + 16, tokens), jnp.bfloat16), pltpu.VMEM((heads, bq), jnp.float32),
                        pltpu.VMEM((heads, HEAD + 16, bq), jnp.float32), pltpu.VMEM((bk, bq), jnp.int32)],
        compiler_params=pltpu.CompilerParams(dimension_semantics=("arbitrary",), vmem_limit_bytes=VMEM),
        cost_estimate=pl.CostEstimate(flops=2 * heads * tokens * tokens * HEAD, transcendentals=heads * tokens * tokens // 2, bytes_accessed=4 * qkv.size),
    )(qkv, qkv, qkv, *turn)


def _attend_back(q_ref, k_ref, v_ref, do_ref, o_ref, lse_ref, cos_ref, sin_ref, out_ref, dq_s, dk_s, dv_s, keys_s, do_s, delta_s, lag_s, *, bk):
    heads, bq = q_ref.shape[:2]
    i = pl.program_id(0)
    scale = HEAD**-0.5
    e = scale * LOG2E
    here = pl.ds(pl.multiple_of(i * bq, bq), bq)

    @pl.when(i == 0)
    def _():
        keys_s[...] = k_ref[...].T
        lag_s[...] = _lag(bk, bq)
        dk_s[...] = jnp.zeros_like(dk_s)
        dv_s[...] = jnp.zeros_like(dv_s)

    dq_s[...] = jnp.zeros_like(dq_s)
    for n in range(heads):
        do = do_ref[:, n * HEAD : (n + 1) * HEAD]
        do_s[n] = do
        both = do.astype(jnp.float32) * o_ref[:, n * HEAD : (n + 1) * HEAD].astype(jnp.float32)
        delta_s[n : n + 1, :] = both.T.sum(axis=0, keepdims=True)

    def block(j, masked):
        keys = pl.ds(pl.multiple_of(j * bk, bk), bk)
        scores = [_dot(k_ref[keys, :], q_ref[n], 1, 1) for n in range(heads)]
        dps = [_dot(v_ref[keys, :], do_s[n], 1, 1) for n in range(heads)]
        for n in range(heads):
            p = jnp.exp2(scores[n] * e - lse_ref[n : n + 1, :])
            if masked:
                p = jnp.where(lag_s[...] >= j * bk - i * bq, p, 0.0)
            ds = (p * (dps[n] - delta_s[n : n + 1, :])).astype(jnp.bfloat16)
            dv_s[keys, :] += _dot(p.astype(jnp.bfloat16), do_s[n], 1, 0)
            dk_s[keys, :] += _dot(ds, q_ref[n], 1, 0)
            dq_s[n] += _dot(keys_s[:, keys], ds, 1, 0)

    whole, last = _blocks(i, bq, bk)
    lax.fori_loop(0, whole, lambda j, _: block(j, False), None)
    lax.fori_loop(whole, last, lambda j, _: block(j, True), None)
    cos, sin = cos_ref[here, :], sin_ref[here, :]
    for n in range(heads):
        dq = (dq_s[n] * scale).T.astype(jnp.bfloat16)
        out_ref[here, n * HEAD : (n + 1) * HEAD] = _turned(dq, cos, -sin)

    @pl.when(i == pl.num_programs(0) - 1)
    def _():
        dk = (dk_s[...] * scale).astype(jnp.bfloat16)
        out_ref[:, heads * HEAD : (heads + 1) * HEAD] = _turned(dk, cos_ref[...], -sin_ref[...])
        out_ref[:, (heads + 1) * HEAD :] = dv_s[...].astype(jnp.bfloat16)


def attend_back(qkv, turned_q, turned_k, by_o, o, lse, turn):
    tokens, heads = qkv.shape[0], qkv.shape[1] // HEAD - 2
    bq, bk = BWD_BLOCK
    column = lambda n: pl.BlockSpec((tokens, HEAD), lambda i: (0, n))
    rows = pl.BlockSpec((bq, heads * HEAD), lambda i: (i, 0))
    return pl.pallas_call(
        functools.partial(_attend_back, bk=bk),
        grid=(tokens // bq,),
        in_specs=[pl.BlockSpec((heads, bq, HEAD), lambda i: (0, i, 0)), column(0), column(heads + 1), rows, rows,
                  pl.BlockSpec((heads, bq), lambda i: (0, i)), column(0), column(0)],
        out_specs=pl.BlockSpec(qkv.shape, lambda i: (0, 0)),
        out_shape=jax.ShapeDtypeStruct(qkv.shape, jnp.bfloat16),
        scratch_shapes=[pltpu.VMEM((heads, HEAD, bq), jnp.float32), pltpu.VMEM((tokens, HEAD), jnp.float32), pltpu.VMEM((tokens, HEAD), jnp.float32),
                        pltpu.VMEM((HEAD, tokens), jnp.bfloat16), pltpu.VMEM((heads, bq, HEAD), jnp.bfloat16), pltpu.VMEM((heads, bq), jnp.float32),
                        pltpu.VMEM((bk, bq), jnp.int32)],
        compiler_params=pltpu.CompilerParams(dimension_semantics=("arbitrary",), vmem_limit_bytes=VMEM),
        cost_estimate=pl.CostEstimate(flops=5 * heads * tokens * tokens * HEAD, transcendentals=heads * tokens * tokens // 2, bytes_accessed=8 * qkv.size),
    )(turned_q, turned_k, qkv, by_o, o, lse, *turn)


UNITS, STRIP = 512, 256


def _strips(tokens, some):
    for at in range(0, tokens, STRIP):
        some(slice(at, at + STRIP))


def _back_of(gate, up, by_act):
    by_act = by_act.astype(jnp.bfloat16).astype(jnp.float32)
    s = jax.nn.sigmoid(gate)
    return (by_act * up * (s + gate * s * (1 - s))).astype(jnp.bfloat16), (by_act * gate * s).astype(jnp.bfloat16)


def _up(b_ref, gate_w, up_w, gate_ref, up_ref, act_ref):
    def some(at):
        gate, up = _dot(b_ref[at, :], gate_w[...], 1, 0), _dot(b_ref[at, :], up_w[...], 1, 0)
        gate_ref[at, :], up_ref[at, :], act_ref[at, :] = gate, up, (gate * jax.nn.sigmoid(gate) * up).astype(jnp.bfloat16)

    _strips(b_ref.shape[0], some)


def _up_and_back(b_ref, by_ref, gate_w, up_w, down_w, act_ref, by_gate, by_up):
    def some(at):
        gate, up = _dot(b_ref[at, :], gate_w[...], 1, 0), _dot(b_ref[at, :], up_w[...], 1, 0)
        act_ref[at, :] = (gate * jax.nn.sigmoid(gate) * up).astype(jnp.bfloat16)
        by_gate[at, :], by_up[at, :] = _back_of(gate, up, _dot(by_ref[at, :], down_w[...], 1, 1))

    _strips(b_ref.shape[0], some)


def _back(by_ref, gate_ref, up_ref, down_w, by_gate, by_up):
    def some(at):
        by_gate[at, :], by_up[at, :] = _back_of(gate_ref[at, :], up_ref[at, :], _dot(by_ref[at, :], down_w[...], 1, 1))

    _strips(by_ref.shape[0], some)


def hidden(kernel, given, outs):
    tokens, units = given[0][1].shape[0], next(a.shape[1] for kind, a in given if kind == "u")
    spec = {"t": lambda a: pl.BlockSpec(a.shape, lambda i: (0, 0)), "u": lambda a: pl.BlockSpec((a.shape[0], UNITS), lambda i: (0, i)),
            "d": lambda a: pl.BlockSpec((UNITS, a.shape[1]), lambda i: (i, 0))}
    return pl.pallas_call(
        kernel,
        grid=(units // UNITS,),
        in_specs=[spec[kind](a) for kind, a in given],
        out_specs=[pl.BlockSpec((tokens, UNITS), lambda i: (0, i)) for _ in outs],
        out_shape=[jax.ShapeDtypeStruct((tokens, units), dtype) for dtype in outs],
        compiler_params=pltpu.CompilerParams(dimension_semantics=("arbitrary",), vmem_limit_bytes=VMEM),
        cost_estimate=pl.CostEstimate(flops=2 * sum(kind != "t" for kind, _ in given) * given[0][1].size * units, transcendentals=tokens * units,
                                      bytes_accessed=sum(2 * a.size for _, a in given) + 4 * len(outs) * tokens * units),
    )(*(a for _, a in given))


MESH = pl.DeviceIdType.MESH
STRIDE = {"x": 8, "y": 4, "z": 2, "c": 1}
ORDER = {"wq": "xyz", "wk": "zxy", "wv": "zxy", "wkv": "zxy", "wo": "yzx", "w_gate": "xyz", "w_up": "yzx", "w_down": "zxy"}


def _here():
    me = lax.axis_index("dp")
    place = {axis: lax.rem(lax.div(me, stride), 2) for axis, stride in STRIDE.items()}
    return me, place, {axis: me + stride * (1 - 2 * place[axis]) for axis, stride in STRIDE.items()}


def _greet(me):
    barrier = pltpu.get_barrier_semaphore()
    for k in range(1, 16):
        pl.semaphore_signal(barrier, inc=1, device_id={"dp": lax.rem(me + k, 16)}, device_id_type=MESH)
    pl.semaphore_wait(barrier, 15)


def _send(src, dst, send_sem, recv_sem, device):
    copy = pltpu.make_async_remote_copy(src_ref=src, dst_ref=dst, send_sem=send_sem, recv_sem=recv_sem, device_id={"dp": device}, device_id_type=MESH)
    copy.start()
    return copy


def _added(out, at, terms, rows, columns):
    wide = _fit(columns, max(28672 // rows, 128))

    def some(c, _):
        here = pl.ds(pl.multiple_of(c * wide, 128), wide)
        total = terms[0][0][terms[0][1], :, here].astype(jnp.float32)
        for ref, i in terms[1:]:
            total += ref[i, :, here].astype(jnp.float32)
        out[at, :, here] = total.astype(jnp.bfloat16)

    lax.fori_loop(0, columns // wide, some, None)


def _scatter(*refs, chains):
    n, arrays = len(chains), 1 + max(which for which, *_ in chains)
    given, squares_ref, (*blocks, total_ref) = refs[:arrays], refs[arrays], refs[arrays + 1 : arrays + n + 2]
    scratch, (square_s, box, load_sem, send_sem, recv_sem, box_send, box_recv) = refs[arrays + n + 2 : -7], refs[-7:]
    half = lambda i, core: given[chains[i][0]].at[:, core, :, pl.ds(chains[i][1], chains[i][2])]
    bufs = [scratch[8 * i : 8 * i + 8] for i in range(n)]
    me, place, near = _here()
    loads = []
    for i in range(n):
        loads.append(pltpu.make_async_copy(half(i, place["c"]), bufs[i][0], load_sem.at[i]))
        loads[i].start()
    _greet(me)
    sent = [[_send(half(i, 1 - place["c"]), bufs[i][1], send_sem.at[i, 0], recv_sem.at[i, 0], near["c"])] for i in range(n)]
    for stage in range(4):
        for i, (*_, order) in enumerate(chains):
            own, core, s1, r1, s2, r2, s3, r3 = bufs[i]
            rows, columns = own.shape[1:]
            w1, w2, w3 = (STRIDE[axis] // 2 for axis in order)
            p1, p2, p3 = (place[axis] for axis in order)
            if stage == 0:
                loads[i].wait()
            sent[i][stage].wait_recv()
            if stage == 0:
                for j in range(4):
                    at = (1 - p1) * w1 + (j // 2) * w2 + (j % 2) * w3
                    _added(s1, j, [(own, at), (core, at)], rows, columns)
                out, into = s1, r1
            elif stage == 1:
                for j in range(2):
                    at = p1 * w1 + (1 - p2) * w2 + j * w3
                    _added(s2, j, [(own, at), (core, at), (r1, (1 - p2) * 2 + j)], rows, columns)
                out, into = s2, r2
            elif stage == 2:
                at = p1 * w1 + p2 * w2 + (1 - p3) * w3
                _added(s3, 0, [(own, at), (core, at), (r1, p2 * 2 + 1 - p3), (r2, 1 - p3)], rows, columns)
                out, into = s3, r3
            else:
                at = p1 * w1 + p2 * w2 + p3 * w3
                _added(blocks[i], 0, [(own, at), (core, at), (r1, p2 * 2 + p3), (r2, p3), (r3, 0)], rows, columns)
            if stage < 3:
                sent[i].append(_send(out, into, send_sem.at[i, stage + 1], recv_sem.at[i, stage + 1], near[order[stage]]))
    squares = jnp.float32(0)
    for i in range(n):
        wide = blocks[i][0].astype(jnp.float32)
        squares += jnp.sum(wide * wide)
    square_s[...] = squares_ref[...] + squares
    copies = [_send(square_s, box.at[k], box_send.at[k], box_recv.at[k], lax.rem(me + k, 16)) for k in range(1, 16)]
    box[0] = square_s[...]
    for copy in copies:
        copy.wait()
    total = jnp.zeros(square_s.shape, jnp.float32)
    for device in range(16):
        total += box[lax.rem(me + 16 - device, 16)]
    total_ref[...] = total
    for each in sent:
        for copy in each:
            copy.wait_send()


def scattered(gradients, chains, squares):
    given = [g.reshape(8, 2, g.shape[0] // 16, g.shape[1]) for g in gradients]
    sizes = [(given[which].shape[2], columns) for which, _, columns, _ in chains]
    scratch = [pltpu.VMEM((count, *size), jnp.bfloat16) for size in sizes for count in (8, 8, 4, 4, 2, 2, 1, 1)]
    n, whole = len(chains), pl.BlockSpec(memory_space=pltpu.VMEM)
    *blocks, total = pl.pallas_call(
        functools.partial(_scatter, chains=chains),
        out_shape=[jax.ShapeDtypeStruct((1, *size), jnp.bfloat16) for size in sizes] + [jax.ShapeDtypeStruct((8, 128), jnp.float32)],
        in_specs=[pl.BlockSpec(memory_space=pl.ANY)] * len(given) + [whole],
        out_specs=[whole] * (n + 1),
        scratch_shapes=scratch + [pltpu.VMEM((8, 128), jnp.float32), pltpu.VMEM((16, 8, 128), jnp.float32)]
        + [pltpu.SemaphoreType.DMA(size) for size in ((n,), (n, 4), (n, 4), (16,), (16,))],
        compiler_params=pltpu.CompilerParams(collective_id=0, has_side_effects=True, vmem_limit_bytes=VMEM),
        cost_estimate=pl.CostEstimate(flops=10**10, transcendentals=0, bytes_accessed=sum(g.size * 2 for g in given)),
    )(*given, jnp.broadcast_to(squares, (8, 128)))
    return [block[0] for block in blocks], total[0, 0]


def _gather(*refs, orders):
    n = len(orders)
    given, outs, (keep_sem, send_sem, recv_sem) = refs[:n], refs[n : 2 * n], refs[-3:]
    me, place, near = _here()
    keeps = []
    for i in range(n):
        keeps.append(pltpu.make_async_copy(given[i], outs[i].at[:, me], keep_sem.at[i]))
        keeps[i].start()
    _greet(me)
    arriving = [{} for _ in orders]
    sent = []
    for stage in range(5):
        for i, order in enumerate(orders):
            path = [*order, "c"]
            held = [()] if stage == 0 else [key for key in arriving[i] if key[-1] == path[stage - 1]]
            for key in held:
                if key:
                    arriving[i][key].wait_recv()
                source = me
                for axis in key:
                    source = source + STRIDE[axis] * (1 - 2 * place[axis])
                src = outs[i].at[:, source] if key else given[i]
                for axis in path[stage:]:
                    k = sum(1 << path.index(other) for other in (*key, axis))
                    arriving[i][(*key, axis)] = _send(src, outs[i].at[:, source], send_sem.at[i, k], recv_sem.at[i, k], near[axis])
                    sent.append(arriving[i][(*key, axis)])
    for copy in sent:
        copy.wait_send()
    for copy in keeps:
        copy.wait()


def gathered(own, names):
    n = len(own)
    outs = pl.pallas_call(
        functools.partial(_gather, orders=[ORDER[name] for name in names]),
        out_shape=[jax.ShapeDtypeStruct((t.shape[0], 16, *t.shape[1:]), t.dtype) for t in own],
        in_specs=[pl.BlockSpec(memory_space=pltpu.VMEM)] * n,
        out_specs=[pl.BlockSpec(memory_space=pl.ANY)] * n,
        scratch_shapes=[pltpu.SemaphoreType.DMA((n,)), pltpu.SemaphoreType.DMA((n, 16)), pltpu.SemaphoreType.DMA((n, 16))],
        compiler_params=pltpu.CompilerParams(collective_id=1, has_side_effects=True, vmem_limit_bytes=VMEM),
        cost_estimate=pl.CostEstimate(flops=10**10, transcendentals=0, bytes_accessed=sum(t.size * 32 for t in own)),
    )(*own)
    outs = pl.pallas_call(
        _moved,
        grid=(8,),
        in_specs=[pl.BlockSpec((t.shape[0], 2, *t.shape[2:]), lambda i: (0, i, 0, 0)) for t in outs],
        out_specs=[pl.BlockSpec((t.shape[0], 2, *t.shape[2:]), lambda i: (0, i, 0, 0)) for t in outs],
        out_shape=[jax.ShapeDtypeStruct(t.shape, t.dtype) for t in outs],
        compiler_params=pltpu.CompilerParams(dimension_semantics=("arbitrary",), vmem_limit_bytes=VMEM),
    )(*outs)
    return [t.reshape(t.shape[0], -1, t.shape[3]) for t in outs]


def _moved(*refs):
    for source, target in zip(refs[: len(refs) // 2], refs[len(refs) // 2 :], strict=True):
        target[...] = source[...]


def matmul(a, w):
    return jnp.dot(a, w, preferred_element_type=jnp.float32).astype(jnp.bfloat16)


def normed(h):
    wide = h.astype(jnp.float32)
    scale = lax.rsqrt(jnp.mean(wide**2, -1, keepdims=True) + 1e-6)
    return (wide * scale).astype(jnp.bfloat16)


def normed_back(h, by_a):
    wide, by_a = h.astype(jnp.float32), by_a.astype(jnp.float32)
    scale = lax.rsqrt(jnp.mean(wide**2, -1, keepdims=True) + 1e-6)
    return (by_a * scale - wide * (scale**3 * jnp.mean(by_a * wide, -1, keepdims=True))).astype(jnp.bfloat16)


def weight_grad(a, g):
    return _dot(a, g, 0, 0).astype(jnp.bfloat16)


def back_through(g, w):
    return _dot(g, w, 1, 1).astype(jnp.bfloat16)


def forward(h, w, turn, by_out):
    a = normed(h)
    qkv = matmul(a, w["qkv"])
    o, lse, turned_q, turned_k = attend(qkv, turn)
    mid = h + matmul(o, w["wo"])
    b = normed(mid)
    if by_out is None:
        gate, up, act = hidden(_up, [("t", b), ("u", w["w_gate"]), ("u", w["w_up"])], [jnp.float32, jnp.float32, jnp.bfloat16])
        return mid + matmul(act, w["w_down"]), (h, a, qkv, o, lse, turned_q, turned_k, mid, b, act, gate, up)
    act, by_gate, by_up = hidden(_up_and_back, [("t", b), ("t", by_out), ("u", w["w_gate"]), ("u", w["w_up"]), ("d", w["w_down"])], [jnp.bfloat16] * 3)
    return None, (h, a, qkv, o, lse, turned_q, turned_k, mid, b, act, by_gate, by_up)


def backward(by_h, kept, w, turn, first, last):
    h, a, qkv, o, lse, turned_q, turned_k, mid, b, act, by_gate, by_up = kept
    if not last:
        by_gate, by_up = hidden(_back, [("t", by_h), ("u", by_gate), ("u", by_up), ("d", w["w_down"])], [jnp.bfloat16] * 2)
    by_w = {"w_down": weight_grad(act, by_h), "w_gate": weight_grad(b, by_gate), "w_up": weight_grad(b, by_up)}
    by_b = back_through(by_gate, w["w_gate"]) + back_through(by_up, w["w_up"])
    by_mid = by_h + normed_back(mid, by_b)
    by_mid, by_w = lax.optimization_barrier((by_mid, by_w))
    by_w["wo"] = weight_grad(o, by_mid)
    by_qkv = attend_back(qkv, turned_q, turned_k, back_through(by_mid, w["wo"]), o, lse, turn)
    by_w["qkv"] = weight_grad(a, by_qkv)
    if first:
        return None, by_w
    by_x = by_mid + normed_back(h, back_through(by_qkv, w["qkv"]))
    return lax.optimization_barrier((by_x, by_w))


def adamw(w, m, v, g):
    m = 0.9 * m + 0.1 * g
    v = 0.95 * v + 0.05 * g * g
    step = m * lax.rsqrt(v + 1e-8) + 0.1 * w
    return (w - 0.02 * step).astype(jnp.bfloat16), m, v


def clipped(gradients, sum_of_squares, count):
    factor = jnp.minimum(1.0, 0.5 * lax.rsqrt(sum_of_squares / count + 1e-30))
    return [g * factor for g in gradients]


def solution(mesh):
    def step(x, dy, *arrays):
        weights, m, v = (arrays[i : i + 7] for i in (0, 7, 14))
        layers, turn = weights[0].shape[0], tables(x.shape[1])
        h, kept, mine = x[0], [], [{} for _ in range(layers)]
        for number in range(layers):
            w = {name: w[number] for name, w in zip(NAMES, weights, strict=True)}
            w["qkv"] = jnp.concatenate([w["wq"], w["wk"], w["wv"]], 1)
            h, saved = forward(h, w, turn, dy[0] if number == layers - 1 else None)
            kept.append((saved, w))
        by_h, grads, chains = dy[0], [], []
        for number in reversed(range(layers)):
            by_h, by_w = backward(by_h, *kept[number], turn, number == 0, number == layers - 1)
            queries = by_w["wo"].shape[0]
            parts = [("wo", "wo", 0, by_w["wo"].shape[1]), ("wq", "qkv", 0, queries), ("wkv", "qkv", queries, 2 * HEAD)]
            if number:
                beside = lambda g: lax.psum_scatter(g, "dp", scatter_dimension=0, tiled=True)
                mine[number]["w_gate"], mine[number]["w_up"] = jnp.split(beside(jnp.concatenate([by_w["w_gate"], by_w["w_up"]], 1)), 2, 1)
                mine[number]["w_down"] = beside(by_w["w_down"])
            else:
                parts = [(name, name, 0, by_w[name].shape[1]) for name in NAMES[4:]] + parts
            for name, source, first, columns in parts:
                if not any(by_w[source] is g for g in grads):
                    grads.append(by_w[source])
                which = next(i for i, g in enumerate(grads) if by_w[source] is g)
                chains.append((number, name, (which, first, columns, ORDER[name])))
        chains.sort(key=lambda chain: chain[0])
        squares = sum(jnp.sum(g.astype(jnp.float32) ** 2) for each in mine for g in each.values())
        blocks, squares = scattered(grads, [chain for *_, chain in chains], squares)
        for (number, name, _), block in zip(chains, blocks, strict=True):
            mine[number][name] = block
        for each in mine:
            each["wk"], each["wv"] = jnp.split(each["wkv"], 2, 1)
        gradients = [jnp.stack([each[name] for each in mine]).astype(jnp.float32) for name in NAMES]
        gradients = clipped(gradients, squares, 16 * sum(g.size for g in gradients))
        me = lax.axis_index("dp")
        own = [lax.dynamic_slice_in_dim(w, me * one.shape[1], one.shape[1], 1).astype(jnp.float32) for w, one in zip(weights, m, strict=True)]
        new = [adamw(w, m, v, g) for w, m, v, g in zip(own, m, v, gradients, strict=True)]
        names = NAMES[4:] + NAMES[:4]
        whole = gathered([new[NAMES.index(name)][0] for name in names], names)
        return (*(whole[names.index(name)] for name in NAMES), *(one[1] for one in new), *(one[2] for one in new))

    states, all_of, cut = P(("rep", "dp"), None, None), P(None, None, None), P(None, "dp", None)
    return jax.shard_map(
        step,
        mesh=mesh,
        in_specs=(states, states) + (all_of,) * 7 + (cut,) * 14,
        out_specs=(P("rep", None, None),) * 7 + (P("rep", "dp", None),) * 14,
        check_vma=False,
    )
```

```python
import functools

import jax
import jax.numpy as jnp
import numpy as np
from jax import lax
from jax.experimental import pallas as pl
from jax.experimental.pallas import tpu as pltpu
from jax.sharding import PartitionSpec as P

NEG = -1e30
LOG2E = 1.4426950408889634
VMEM = 56 * 2**20
HEAD = 128
THETA = 10000
NAMES = ("wq", "wk", "wv", "wo", "w_gate", "w_up", "w_down")
FWD_BLOCK, BWD_BLOCK = (512, 512), (512, 512)


def _fit(size, want, unit=128):
    return max(n for n in range(unit, max(min(want, size), unit) + 1, unit) if size % n == 0)


def _dot(a, b, ca, cb):
    return lax.dot_general(a, b, (((ca,), (cb,)), ((), ())), preferred_element_type=jnp.float32)


def tables(tokens):
    half = HEAD // 2
    angle = np.arange(tokens)[:, None] * float(THETA) ** (-np.arange(half) / half)
    cos, sin = np.cos(angle), np.sin(angle)
    return jnp.asarray(np.concatenate([cos, cos], 1), jnp.float32), jnp.asarray(np.concatenate([-sin, sin], 1), jnp.float32)


def _turned(t, cos, sin):
    wide = t.astype(jnp.float32)
    return (wide * cos + pltpu.roll(wide, HEAD // 2, 1) * sin).astype(jnp.bfloat16)


def _blocks(i, bq, bk):
    return lax.div(i * bq, bk), lax.div(i * bq + bq + bk - 1, bk)


def _lag(bk, bq):
    return lax.broadcasted_iota(jnp.int32, (bk, bq), 1) - lax.broadcasted_iota(jnp.int32, (bk, bq), 0)


def _attend(q_ref, k_ref, v_ref, cos_ref, sin_ref, o_ref, lse_ref, turned_ref, key_ref, values_s, top_s, mix_s, lag_s, *, bk):
    bq, heads = q_ref.shape[0], q_ref.shape[1] // HEAD
    i = pl.program_id(0)
    scale = HEAD**-0.5
    e = scale * LOG2E
    here = pl.ds(pl.multiple_of(i * bq, bq), bq)

    @pl.when(i == 0)
    def _():
        key_ref[...] = _turned(k_ref[...], cos_ref[...], sin_ref[...])
        values_s[:HEAD, :] = v_ref[...].T
        values_s[HEAD:, :] = jnp.ones((16, v_ref.shape[0]), jnp.bfloat16)
        lag_s[...] = _lag(bk, bq)

    cos, sin = cos_ref[here, :], sin_ref[here, :]
    for n in range(heads):
        turned_ref[n] = _turned(q_ref[:, n * HEAD : (n + 1) * HEAD], cos, sin)
    top_s[...] = jnp.full(top_s.shape, NEG, jnp.float32)
    mix_s[...] = jnp.zeros(mix_s.shape, jnp.float32)

    def block(j, masked):
        keys = pl.ds(pl.multiple_of(j * bk, bk), bk)
        scores = [_dot(key_ref[keys, :], turned_ref[n], 1, 1) for n in range(heads)]
        weights, keeps = [], []
        for n, s in enumerate(scores):
            if masked:
                s = jnp.where(lag_s[...] >= j * bk - i * bq, s, 2 * NEG)
            old = top_s[n : n + 1, :]
            top = jnp.maximum(old, s.max(axis=0, keepdims=True))
            top_s[n : n + 1, :] = top
            weights.append(jnp.exp2((s - top) * e).astype(jnp.bfloat16))
            keeps.append(jnp.exp2((old - top) * e))
        for n, (p, keep) in enumerate(zip(weights, keeps)):
            mix_s[n] = mix_s[n] * keep + _dot(values_s[:, keys], p, 1, 0)

    whole, last = _blocks(i, bq, bk)
    lax.fori_loop(0, whole, lambda j, _: block(j, False), None)
    lax.fori_loop(whole, last, lambda j, _: block(j, True), None)
    for n in range(heads):
        total = mix_s[n, HEAD : HEAD + 1, :]
        o_ref[:, n * HEAD : (n + 1) * HEAD] = (mix_s[n, :HEAD, :] * (1 / total)).T.astype(o_ref.dtype)
        lse_ref[n : n + 1, :] = top_s[n : n + 1, :] * e + jnp.log2(total)


def attend(qkv, turn):
    tokens, heads = qkv.shape[0], qkv.shape[1] // HEAD - 2
    bq, bk = FWD_BLOCK
    column = lambda n: pl.BlockSpec((tokens, HEAD), lambda i: (0, n))
    rows = pl.BlockSpec((bq, heads * HEAD), lambda i: (i, 0))
    return pl.pallas_call(
        functools.partial(_attend, bk=bk),
        grid=(tokens // bq,),
        in_specs=[rows, column(heads), column(heads + 1), column(0), column(0)],
        out_specs=[rows, pl.BlockSpec((heads, bq), lambda i: (0, i)), pl.BlockSpec((heads, bq, HEAD), lambda i: (0, i, 0)), column(0)],
        out_shape=[jax.ShapeDtypeStruct((tokens, heads * HEAD), jnp.bfloat16), jax.ShapeDtypeStruct((heads, tokens), jnp.float32),
                   jax.ShapeDtypeStruct((heads, tokens, HEAD), jnp.bfloat16), jax.ShapeDtypeStruct((tokens, HEAD), jnp.bfloat16)],
        scratch_shapes=[pltpu.VMEM((HEAD + 16, tokens), jnp.bfloat16), pltpu.VMEM((heads, bq), jnp.float32),
                        pltpu.VMEM((heads, HEAD + 16, bq), jnp.float32), pltpu.VMEM((bk, bq), jnp.int32)],
        compiler_params=pltpu.CompilerParams(dimension_semantics=("arbitrary",), vmem_limit_bytes=VMEM),
        cost_estimate=pl.CostEstimate(flops=2 * heads * tokens * tokens * HEAD, transcendentals=heads * tokens * tokens // 2, bytes_accessed=4 * qkv.size),
    )(qkv, qkv, qkv, *turn)


def _attend_back(q_ref, k_ref, v_ref, do_ref, o_ref, lse_ref, cos_ref, sin_ref, out_ref, dq_s, dk_s, dv_s, keys_s, do_s, delta_s, lag_s, *, bk):
    heads, bq = q_ref.shape[:2]
    i = pl.program_id(0)
    scale = HEAD**-0.5
    e = scale * LOG2E
    here = pl.ds(pl.multiple_of(i * bq, bq), bq)

    @pl.when(i == 0)
    def _():
        keys_s[...] = k_ref[...].T
        lag_s[...] = _lag(bk, bq)
        dk_s[...] = jnp.zeros_like(dk_s)
        dv_s[...] = jnp.zeros_like(dv_s)

    dq_s[...] = jnp.zeros_like(dq_s)
    for n in range(heads):
        do = do_ref[:, n * HEAD : (n + 1) * HEAD]
        do_s[n] = do
        both = do.astype(jnp.float32) * o_ref[:, n * HEAD : (n + 1) * HEAD].astype(jnp.float32)
        delta_s[n : n + 1, :] = both.T.sum(axis=0, keepdims=True)

    def block(j, masked):
        keys = pl.ds(pl.multiple_of(j * bk, bk), bk)
        scores = [_dot(k_ref[keys, :], q_ref[n], 1, 1) for n in range(heads)]
        dps = [_dot(v_ref[keys, :], do_s[n], 1, 1) for n in range(heads)]
        for n in range(heads):
            p = jnp.exp2(scores[n] * e - lse_ref[n : n + 1, :])
            if masked:
                p = jnp.where(lag_s[...] >= j * bk - i * bq, p, 0.0)
            ds = (p * (dps[n] - delta_s[n : n + 1, :])).astype(jnp.bfloat16)
            dv_s[keys, :] += _dot(p.astype(jnp.bfloat16), do_s[n], 1, 0)
            dk_s[keys, :] += _dot(ds, q_ref[n], 1, 0)
            dq_s[n] += _dot(keys_s[:, keys], ds, 1, 0)

    whole, last = _blocks(i, bq, bk)
    lax.fori_loop(0, whole, lambda j, _: block(j, False), None)
    lax.fori_loop(whole, last, lambda j, _: block(j, True), None)
    cos, sin = cos_ref[here, :], sin_ref[here, :]
    for n in range(heads):
        dq = (dq_s[n] * scale).T.astype(jnp.bfloat16)
        out_ref[here, n * HEAD : (n + 1) * HEAD] = _turned(dq, cos, -sin)

    @pl.when(i == pl.num_programs(0) - 1)
    def _():
        dk = (dk_s[...] * scale).astype(jnp.bfloat16)
        out_ref[:, heads * HEAD : (heads + 1) * HEAD] = _turned(dk, cos_ref[...], -sin_ref[...])
        out_ref[:, (heads + 1) * HEAD :] = dv_s[...].astype(jnp.bfloat16)


def attend_back(qkv, turned_q, turned_k, by_o, o, lse, turn):
    tokens, heads = qkv.shape[0], qkv.shape[1] // HEAD - 2
    bq, bk = BWD_BLOCK
    column = lambda n: pl.BlockSpec((tokens, HEAD), lambda i: (0, n))
    rows = pl.BlockSpec((bq, heads * HEAD), lambda i: (i, 0))
    return pl.pallas_call(
        functools.partial(_attend_back, bk=bk),
        grid=(tokens // bq,),
        in_specs=[pl.BlockSpec((heads, bq, HEAD), lambda i: (0, i, 0)), column(0), column(heads + 1), rows, rows,
                  pl.BlockSpec((heads, bq), lambda i: (0, i)), column(0), column(0)],
        out_specs=pl.BlockSpec(qkv.shape, lambda i: (0, 0)),
        out_shape=jax.ShapeDtypeStruct(qkv.shape, jnp.bfloat16),
        scratch_shapes=[pltpu.VMEM((heads, HEAD, bq), jnp.float32), pltpu.VMEM((tokens, HEAD), jnp.float32), pltpu.VMEM((tokens, HEAD), jnp.float32),
                        pltpu.VMEM((HEAD, tokens), jnp.bfloat16), pltpu.VMEM((heads, bq, HEAD), jnp.bfloat16), pltpu.VMEM((heads, bq), jnp.float32),
                        pltpu.VMEM((bk, bq), jnp.int32)],
        compiler_params=pltpu.CompilerParams(dimension_semantics=("arbitrary",), vmem_limit_bytes=VMEM),
        cost_estimate=pl.CostEstimate(flops=5 * heads * tokens * tokens * HEAD, transcendentals=heads * tokens * tokens // 2, bytes_accessed=8 * qkv.size),
    )(turned_q, turned_k, qkv, by_o, o, lse, *turn)


UNITS, STRIP = 256, 256


def _strips(tokens, some):
    for at in range(0, tokens, STRIP):
        some(slice(at, at + STRIP))


def _back_of(gate, up, by_act):
    by_act = by_act.astype(jnp.bfloat16).astype(jnp.float32)
    s = jax.nn.sigmoid(gate)
    by_s = by_act * s
    return (by_s * up * (1 + gate * (1 - s))).astype(jnp.bfloat16), (by_s * gate).astype(jnp.bfloat16)


def _up(b_ref, gate_w, up_w, gate_ref, up_ref, act_ref):
    def some(at):
        gate, up = _dot(b_ref[at, :], gate_w[...], 1, 0), _dot(b_ref[at, :], up_w[...], 1, 0)
        gate_ref[at, :], up_ref[at, :], act_ref[at, :] = gate, up, (gate * jax.nn.sigmoid(gate) * up).astype(jnp.bfloat16)

    _strips(b_ref.shape[0], some)


def _up_and_back(b_ref, by_ref, gate_w, up_w, down_w, act_ref, by_gate, by_up):
    def some(at):
        gate, up = _dot(b_ref[at, :], gate_w[...], 1, 0), _dot(b_ref[at, :], up_w[...], 1, 0)
        act_ref[at, :] = (gate * jax.nn.sigmoid(gate) * up).astype(jnp.bfloat16)
        by_gate[at, :], by_up[at, :] = _back_of(gate, up, _dot(by_ref[at, :], down_w[...], 1, 1))

    _strips(b_ref.shape[0], some)


def _back(by_ref, gate_ref, up_ref, down_w, by_gate, by_up):
    def some(at):
        by_gate[at, :], by_up[at, :] = _back_of(gate_ref[at, :], up_ref[at, :], _dot(by_ref[at, :], down_w[...], 1, 1))

    _strips(by_ref.shape[0], some)


def hidden(kernel, given, outs, number):
    tokens, units = given[0][1].shape[0], next(a.shape[1] for kind, a in given if kind == "d") if given[-1][0] == "d" else given[-1][1].shape[2]
    spec = {"t": lambda a: pl.BlockSpec(a.shape, lambda i: (0, 0)), "h": lambda a: pl.BlockSpec((tokens, UNITS), lambda i: (0, i)),
            "u": lambda a: pl.BlockSpec((None, a.shape[1], UNITS), lambda i: (number, 0, i)),
            "d": lambda a: pl.BlockSpec((None, UNITS, a.shape[2]), lambda i: (number, i, 0))}
    return pl.pallas_call(
        kernel,
        grid=(units // UNITS,),
        in_specs=[spec[kind](a) for kind, a in given],
        out_specs=[pl.BlockSpec((tokens, UNITS), lambda i: (0, i)) for _ in outs],
        out_shape=[jax.ShapeDtypeStruct((tokens, units), dtype) for dtype in outs],
        compiler_params=pltpu.CompilerParams(dimension_semantics=("arbitrary",), vmem_limit_bytes=VMEM),
        cost_estimate=pl.CostEstimate(flops=2 * sum(kind != "t" for kind, _ in given) * given[0][1].size * units, transcendentals=tokens * units,
                                      bytes_accessed=sum(2 * a.size for _, a in given) + 4 * len(outs) * tokens * units),
    )(*(a for _, a in given))


def _projected(t_ref, w_ref, h_ref, out_ref, normed_ref):
    def some(at):
        added = h_ref[at, :] + _dot(t_ref[at, :], w_ref[...], 1, 0).astype(jnp.bfloat16)
        out_ref[at, :], normed_ref[at, :] = added, normed(added)

    _strips(h_ref.shape[0], some)


def projected(t, w, number, h):
    rows = lambda a: pl.BlockSpec((2 * STRIP, a.shape[1]), lambda i: (i, 0))
    return pl.pallas_call(
        _projected,
        grid=(h.shape[0] // (2 * STRIP),),
        in_specs=[rows(t), pl.BlockSpec((None, *w.shape[1:]), lambda i: (number, 0, 0)), rows(h)],
        out_specs=[rows(h)] * 2,
        out_shape=[jax.ShapeDtypeStruct(h.shape, h.dtype)] * 2,
        compiler_params=pltpu.CompilerParams(dimension_semantics=("arbitrary",), vmem_limit_bytes=VMEM),
        cost_estimate=pl.CostEstimate(flops=2 * t.size * h.shape[1], transcendentals=0, bytes_accessed=2 * t.size + 6 * h.size),
    )(t, w, h)


MESH = pl.DeviceIdType.MESH
STRIDE = {"x": 8, "y": 4, "z": 2, "c": 1}
ORDER = {"wq": "xyz", "wk": "zxy", "wv": "zxy", "wkv": "zxy", "wo": "yzx", "w_gate": "xyz", "w_up": "yzx", "w_down": "zxy"}


def _here():
    me = lax.axis_index("dp")
    place = {axis: lax.rem(lax.div(me, stride), 2) for axis, stride in STRIDE.items()}
    return me, place, {axis: me + stride * (1 - 2 * place[axis]) for axis, stride in STRIDE.items()}


def _greet(me):
    barrier = pltpu.get_barrier_semaphore()
    for k in range(1, 16):
        pl.semaphore_signal(barrier, inc=1, device_id={"dp": lax.rem(me + k, 16)}, device_id_type=MESH)
    pl.semaphore_wait(barrier, 15)


def _send(src, dst, send_sem, recv_sem, device):
    copy = pltpu.make_async_remote_copy(src_ref=src, dst_ref=dst, send_sem=send_sem, recv_sem=recv_sem, device_id={"dp": device}, device_id_type=MESH)
    copy.start()
    return copy


def _added(out, at, terms, rows, columns):
    wide = _fit(columns, max(28672 // rows, 128))

    def some(c, _):
        here = pl.ds(pl.multiple_of(c * wide, 128), wide)
        total = terms[0][0][terms[0][1], :, here].astype(jnp.float32)
        for ref, i in terms[1:]:
            total += ref[i, :, here].astype(jnp.float32)
        out[at, :, here] = total.astype(jnp.bfloat16)

    lax.fori_loop(0, columns // wide, some, None)


def _scatter(*refs, chains):
    n, arrays = len(chains), 1 + max(which for which, *_ in chains)
    given, squares_ref, (*blocks, total_ref) = refs[:arrays], refs[arrays], refs[arrays + 1 : arrays + n + 2]
    scratch, (square_s, box, load_sem, send_sem, recv_sem, box_send, box_recv) = refs[arrays + n + 2 : -7], refs[-7:]
    half = lambda i, core: given[chains[i][0]].at[:, core, :, pl.ds(chains[i][1], chains[i][2])]
    bufs = [scratch[8 * i : 8 * i + 8] for i in range(n)]
    me, place, near = _here()
    loads = []
    for i in range(n):
        loads.append(pltpu.make_async_copy(half(i, place["c"]), bufs[i][0], load_sem.at[i]))
        loads[i].start()
    _greet(me)
    sent = [[_send(half(i, 1 - place["c"]), bufs[i][1], send_sem.at[i, 0], recv_sem.at[i, 0], near["c"])] for i in range(n)]
    for stage in range(4):
        for i, (*_, order) in enumerate(chains):
            own, core, s1, r1, s2, r2, s3, r3 = bufs[i]
            rows, columns = own.shape[1:]
            w1, w2, w3 = (STRIDE[axis] // 2 for axis in order)
            p1, p2, p3 = (place[axis] for axis in order)
            if stage == 0:
                loads[i].wait()
            sent[i][stage].wait_recv()
            if stage == 0:
                for j in range(4):
                    at = (1 - p1) * w1 + (j // 2) * w2 + (j % 2) * w3
                    _added(s1, j, [(own, at), (core, at)], rows, columns)
                out, into = s1, r1
            elif stage == 1:
                for j in range(2):
                    at = p1 * w1 + (1 - p2) * w2 + j * w3
                    _added(s2, j, [(own, at), (core, at), (r1, (1 - p2) * 2 + j)], rows, columns)
                out, into = s2, r2
            elif stage == 2:
                at = p1 * w1 + p2 * w2 + (1 - p3) * w3
                _added(s3, 0, [(own, at), (core, at), (r1, p2 * 2 + 1 - p3), (r2, 1 - p3)], rows, columns)
                out, into = s3, r3
            else:
                at = p1 * w1 + p2 * w2 + p3 * w3
                _added(blocks[i], 0, [(own, at), (core, at), (r1, p2 * 2 + p3), (r2, p3), (r3, 0)], rows, columns)
            if stage < 3:
                sent[i].append(_send(out, into, send_sem.at[i, stage + 1], recv_sem.at[i, stage + 1], near[order[stage]]))
    squares = jnp.float32(0)
    for i in range(n):
        wide = blocks[i][0].astype(jnp.float32)
        squares += jnp.sum(wide * wide)
    square_s[...] = squares_ref[...] + squares
    copies = [_send(square_s, box.at[k], box_send.at[k], box_recv.at[k], lax.rem(me + k, 16)) for k in range(1, 16)]
    box[0] = square_s[...]
    for copy in copies:
        copy.wait()
    total = jnp.zeros(square_s.shape, jnp.float32)
    for device in range(16):
        total += box[lax.rem(me + 16 - device, 16)]
    total_ref[...] = total
    for each in sent:
        for copy in each:
            copy.wait_send()


def scattered(gradients, chains, squares):
    given = [g.reshape(8, 2, g.shape[0] // 16, g.shape[1]) for g in gradients]
    sizes = [(given[which].shape[2], columns) for which, _, columns, _ in chains]
    scratch = [pltpu.VMEM((count, *size), jnp.bfloat16) for size in sizes for count in (8, 8, 4, 4, 2, 2, 1, 1)]
    n, whole = len(chains), pl.BlockSpec(memory_space=pltpu.VMEM)
    *blocks, total = pl.pallas_call(
        functools.partial(_scatter, chains=chains),
        out_shape=[jax.ShapeDtypeStruct((1, *size), jnp.bfloat16) for size in sizes] + [jax.ShapeDtypeStruct((8, 128), jnp.float32)],
        in_specs=[pl.BlockSpec(memory_space=pl.ANY)] * len(given) + [whole],
        out_specs=[whole] * (n + 1),
        scratch_shapes=scratch + [pltpu.VMEM((8, 128), jnp.float32), pltpu.VMEM((16, 8, 128), jnp.float32)]
        + [pltpu.SemaphoreType.DMA(size) for size in ((n,), (n, 4), (n, 4), (16,), (16,))],
        compiler_params=pltpu.CompilerParams(collective_id=0, has_side_effects=True, vmem_limit_bytes=VMEM),
        cost_estimate=pl.CostEstimate(flops=10**10, transcendentals=0, bytes_accessed=sum(g.size * 2 for g in given)),
    )(*given, jnp.broadcast_to(squares, (8, 128)))
    return [block[0] for block in blocks], total[0, 0]


def _gather(*refs, orders):
    n = len(orders)
    given, outs, (keep_sem, send_sem, recv_sem) = refs[:n], refs[n : 2 * n], refs[-3:]
    me, place, near = _here()
    keeps = []
    for i in range(n):
        keeps.append(pltpu.make_async_copy(given[i], outs[i].at[:, me], keep_sem.at[i]))
        keeps[i].start()
    _greet(me)
    arriving = [{} for _ in orders]
    sent = []
    for stage in range(5):
        for i, order in enumerate(orders):
            path = [*order, "c"]
            held = [()] if stage == 0 else [key for key in arriving[i] if key[-1] == path[stage - 1]]
            for key in held:
                if key:
                    arriving[i][key].wait_recv()
                source = me
                for axis in key:
                    source = source + STRIDE[axis] * (1 - 2 * place[axis])
                src = outs[i].at[:, source] if key else given[i]
                for axis in path[stage:]:
                    k = sum(1 << path.index(other) for other in (*key, axis))
                    arriving[i][(*key, axis)] = _send(src, outs[i].at[:, source], send_sem.at[i, k], recv_sem.at[i, k], near[axis])
                    sent.append(arriving[i][(*key, axis)])
    for copy in sent:
        copy.wait_send()
    for copy in keeps:
        copy.wait()


def gathered(own, names):
    n = len(own)
    outs = pl.pallas_call(
        functools.partial(_gather, orders=[ORDER[name] for name in names]),
        out_shape=[jax.ShapeDtypeStruct((t.shape[0], 16, *t.shape[1:]), t.dtype) for t in own],
        in_specs=[pl.BlockSpec(memory_space=pltpu.VMEM)] * n,
        out_specs=[pl.BlockSpec(memory_space=pl.ANY)] * n,
        scratch_shapes=[pltpu.SemaphoreType.DMA((n,)), pltpu.SemaphoreType.DMA((n, 16)), pltpu.SemaphoreType.DMA((n, 16))],
        compiler_params=pltpu.CompilerParams(collective_id=1, has_side_effects=True, vmem_limit_bytes=VMEM),
        cost_estimate=pl.CostEstimate(flops=10**10, transcendentals=0, bytes_accessed=sum(t.size * 32 for t in own)),
    )(*own)
    outs = pl.pallas_call(
        _moved,
        grid=(8,),
        in_specs=[pl.BlockSpec((t.shape[0], 2, *t.shape[2:]), lambda i: (0, i, 0, 0)) for t in outs],
        out_specs=[pl.BlockSpec((t.shape[0], 2, *t.shape[2:]), lambda i: (0, i, 0, 0)) for t in outs],
        out_shape=[jax.ShapeDtypeStruct(t.shape, t.dtype) for t in outs],
        compiler_params=pltpu.CompilerParams(dimension_semantics=("arbitrary",), vmem_limit_bytes=VMEM),
    )(*outs)
    return [t.reshape(t.shape[0], -1, t.shape[3]) for t in outs]


def _moved(*refs):
    for source, target in zip(refs[: len(refs) // 2], refs[len(refs) // 2 :], strict=True):
        target[...] = source[...]


def matmul(a, w):
    return jnp.dot(a, w, preferred_element_type=jnp.float32).astype(jnp.bfloat16)


def normed(h):
    wide = h.astype(jnp.float32)
    scale = lax.rsqrt(jnp.mean(wide**2, -1, keepdims=True) + 1e-6)
    return (wide * scale).astype(jnp.bfloat16)


def normed_back(h, by_a):
    wide, by_a = h.astype(jnp.float32), by_a.astype(jnp.float32)
    scale = lax.rsqrt(jnp.mean(wide**2, -1, keepdims=True) + 1e-6)
    return (by_a * scale - wide * (scale**3 * jnp.mean(by_a * wide, -1, keepdims=True))).astype(jnp.bfloat16)


def weight_grad(a, g):
    return _dot(a, g, 0, 0).astype(jnp.bfloat16)


def back_through(g, w):
    return _dot(g, w, 1, 1).astype(jnp.bfloat16)


def forward(h, a, w, number, turn, by_out):
    qkv = matmul(a, w["qkv"][number])
    o, lse, turned_q, turned_k = attend(qkv, turn)
    mid, b = projected(o, w["wo"], number, h)
    ups = [("u", w["w_gate"]), ("u", w["w_up"])]
    if by_out is None:
        gate, up, act = hidden(_up, [("t", b), *ups], [jnp.float32, jnp.float32, jnp.bfloat16], number)
        return *projected(act, w["w_down"], number, mid), (h, a, qkv, o, lse, turned_q, turned_k, mid, b, act, gate, up)
    act, by_gate, by_up = hidden(_up_and_back, [("t", b), ("t", by_out), *ups, ("d", w["w_down"])], [jnp.bfloat16] * 3, number)
    return None, None, (h, a, qkv, o, lse, turned_q, turned_k, mid, b, act, by_gate, by_up)


def backward(by_h, kept, w, number, turn, last):
    h, a, qkv, o, lse, turned_q, turned_k, mid, b, act, by_gate, by_up = kept
    if not last:
        by_gate, by_up = hidden(_back, [("t", by_h), ("h", by_gate), ("h", by_up), ("d", w["w_down"])], [jnp.bfloat16] * 2, number)
    by_w = {"w_down": weight_grad(act, by_h), "w_gate": weight_grad(b, by_gate), "w_up": weight_grad(b, by_up)}
    by_b = back_through(by_gate, w["w_gate"][number]) + back_through(by_up, w["w_up"][number])
    by_mid = by_h + normed_back(mid, by_b)
    by_mid, by_w = lax.optimization_barrier((by_mid, by_w))
    by_w["wo"] = weight_grad(o, by_mid)
    by_qkv = attend_back(qkv, turned_q, turned_k, back_through(by_mid, w["wo"][number]), o, lse, turn)
    by_w["qkv"] = weight_grad(a, by_qkv)
    if number == 0:
        return None, by_w
    by_x = by_mid + normed_back(h, back_through(by_qkv, w["qkv"][number]))
    return lax.optimization_barrier((by_x, by_w))


def adamw(w, m, v, g):
    m = 0.9 * m + 0.1 * g
    v = 0.95 * v + 0.05 * g * g
    step = m * lax.rsqrt(v + 1e-8) + 0.1 * w
    return (w - 0.02 * step).astype(jnp.bfloat16), m, v


def clipped(gradients, sum_of_squares, count):
    factor = jnp.minimum(1.0, 0.5 * lax.rsqrt(sum_of_squares / count + 1e-30))
    return [g * factor for g in gradients]


def solution(mesh):
    def step(x, dy, *arrays):
        weights, m, v = (arrays[i : i + 7] for i in (0, 7, 14))
        layers, turn = weights[0].shape[0], tables(x.shape[1])
        w = dict(zip(NAMES, weights, strict=True))
        w["qkv"] = [jnp.concatenate([w[name][number] for name in NAMES[:3]], 1) for number in range(layers)]
        h, a, kept, mine = x[0], normed(x[0]), [], [{} for _ in range(layers)]
        for number in range(layers):
            h, a, saved = forward(h, a, w, number, turn, dy[0] if number == layers - 1 else None)
            kept.append(saved)
        by_h, grads, chains = dy[0], [], []
        for number in reversed(range(layers)):
            by_h, by_w = backward(by_h, kept[number], w, number, turn, number == layers - 1)
            queries = by_w["wo"].shape[0]
            parts = [("wo", "wo", 0, by_w["wo"].shape[1]), ("wq", "qkv", 0, queries), ("wkv", "qkv", queries, 2 * HEAD)]
            if number:
                for name in NAMES[4:]:
                    mine[number][name] = lax.psum_scatter(by_w[name], "dp", scatter_dimension=0, tiled=True)
            else:
                parts = [(name, name, 0, by_w[name].shape[1]) for name in NAMES[4:]] + parts
            for name, source, first, columns in parts:
                if not any(by_w[source] is g for g in grads):
                    grads.append(by_w[source])
                which = next(i for i, g in enumerate(grads) if by_w[source] is g)
                chains.append((number, name, (which, first, columns, ORDER[name])))
        squares = sum(jnp.sum(g.astype(jnp.float32) ** 2) for each in mine for g in each.values())
        blocks, squares = scattered(grads, [chain for *_, chain in chains], squares)
        for (number, name, _), block in zip(chains, blocks, strict=True):
            mine[number][name] = block
        for each in mine:
            each["wk"], each["wv"] = jnp.split(each["wkv"], 2, 1)
        gradients = [jnp.stack([each[name] for each in mine]).astype(jnp.float32) for name in NAMES]
        gradients = clipped(gradients, squares, 16 * sum(g.size for g in gradients))
        me = lax.axis_index("dp")
        own = [lax.dynamic_slice_in_dim(w, me * one.shape[1], one.shape[1], 1).astype(jnp.float32) for w, one in zip(weights, m, strict=True)]
        new = [adamw(w, m, v, g) for w, m, v, g in zip(own, m, v, gradients, strict=True)]
        names = NAMES[4:] + NAMES[:4]
        whole = gathered([new[NAMES.index(name)][0] for name in names], names)
        return (*(whole[names.index(name)] for name in NAMES), *(one[1] for one in new), *(one[2] for one in new))

    states, all_of, cut = P(("rep", "dp"), None, None), P(None, None, None), P(None, "dp", None)
    return jax.shard_map(
        step,
        mesh=mesh,
        in_specs=(states, states) + (all_of,) * 7 + (cut,) * 14,
        out_specs=(P("rep", None, None),) * 7 + (P("rep", "dp", None),) * 14,
        check_vma=False,
    )
```
